32 devices in a mesh: obs: 8 (over z, x), chan: 4 (over y, core).
Axes of the slice: x: 2, y: 2, z: 4, core: 2. Of those that a mesh axis runs over, the one named last changes fastest.
Arguments:
- departures: bfloat16 [8192, 16384], P('chan', 'obs'), may hold values from -8 to 8
- predictors: bfloat16 [10, 16384], P(None, 'obs'), may hold values from -3 to 3
- inv_band: bfloat16 [63, 8192], P(None, 'chan'), may hold values from -1 to 2.5
- band_id: int32 [8192], replicated, may hold values from 0 to 340, never falling along the last dimension, each value on 1 to 32 neighbouring positions
- line_counts: int32 [128], P('obs'), may hold values from 24 to 128
Outputs:
- gram: float32 [100, 8192], P(None, ('chan', 'obs'))
- rhs: float32 [10, 8192], P(None, ('chan', 'obs'))
The draws below stay inside these ranges and needn't reach their ends.
Inputs may be any that keep to these rules, and one draw needn't show every extreme that they name: `band_id`: band numbers never fall along the channels; a band spans 1 to 32 channels. `line_counts`: slots of a scan line at or beyond its count are empty.
All inputs are finite; a program needn't handle non-finite values.
Results may differ from the reference program's by a relative error of at most 0.00062.
Values may be sent and summed in bfloat16 or wider, within the bound.
A program may use at most 64 MiB of HBM per device.

```python
import math
import jax
import jax.numpy as jnp
import numpy as np
from jax import lax

P_SIZE = 10
C = 8192
MAXB = 32
LINE_SLOTS = 128
LINES = 128
NOBS = 16384


def draw_inv_band(key, part):
    first_key, second_key = jax.random.split(jax.random.fold_in(key, 17))
    coupling = jnp.clip(0.2 * jax.random.normal(first_key, (2 * MAXB - 1, C), jnp.float32), -1.0, 1.0)
    center = jnp.exp(jax.random.uniform(second_key, (C,), jnp.float32, jnp.log(0.5), jnp.log(2.0)))
    rows_at = jnp.arange(2 * MAXB - 1)[:, None]
    return jnp.where(rows_at == MAXB - 1, center[None, :], coupling).astype(jnp.bfloat16)


def observation_predictors(key):
    value_key = jax.random.fold_in(jax.random.fold_in(key, 101), 1)
    place = jnp.arange(NOBS, dtype=jnp.float32) / jnp.float32(NOBS)
    rising = 0.7 * jnp.exp(jnp.log(3.0) * place)
    level = rising
    values = jax.random.uniform(value_key, (P_SIZE, NOBS), jnp.float32, -1.0, 1.0)
    return values * level[None, :]


def draw_predictors(key, part):
    return observation_predictors(key).astype(jnp.bfloat16)


def draw_departures(key, part):
    pred = observation_predictors(key)
    coef_key, scale_key, noise_key = jax.random.split(jax.random.fold_in(key, 202), 3)
    scales = jnp.exp(jax.random.uniform(scale_key, (C,), jnp.float32, jnp.log(0.2), jnp.log(1.2)))
    coefs = 0.5 * jax.random.normal(coef_key, (C, P_SIZE), jnp.float32) * scales[:, None]
    block = 128
    coef_blocks = coefs.reshape(C // block, block, P_SIZE)

    def one_block(index):
        bias = jnp.dot(coef_blocks[index], pred, precision=lax.Precision.HIGHEST)
        block_key = jax.random.fold_in(noise_key, index)
        noise = 0.5 * jax.random.normal(block_key, (block, NOBS), jnp.float32)
        return jnp.clip(bias + noise, -8.0, 8.0).astype(jnp.bfloat16)
    blocks = lax.map(one_block, jnp.arange(C // block, dtype=jnp.int32))
    return blocks.reshape(C, NOBS)


def set_ends(result, stream_key, smallest, largest):
    shape = result.shape
    spot = [jax.random.randint(jax.random.fold_in(stream_key, axis), (), 0, shape[axis]) for axis in range(len(shape))]
    result = result.at[tuple(spot)].set(smallest)
    longest = shape.index(max(shape))
    spot[longest] = (spot[longest] + 1) % shape[longest]
    return result.at[tuple(spot)].set(largest)


def split_up(count, total, most, skew):
    weights = [(1 << 20) // math.isqrt(grade ** skew) + 1 for grade in range(2, count + 1)]
    surplus, holding = total - most - (count - 1), [1] * (count - 1)
    while surplus > 0:
        free = [i for i in range(count - 1) if holding[i] < most]
        mass, remaining = sum([weights[i] for i in free]), surplus
        for i in free:
            addition = min(most - holding[i], max(1, remaining * weights[i] // mass), surplus)
            holding[i] = holding[i] + addition
            surplus = surplus - addition
    return np.array([most] + holding)


def ragged(stream_key, number_of, total, most, skew):
    if number_of == 2:
        one = jax.random.randint(stream_key, (), max(1, total - most), min(most, total - 1) + 1)
        return jnp.stack([one, total - one])
    lengths = jnp.asarray(split_up(number_of, total, most, skew), jnp.int32)
    pairs = (number_of - 1) // 2
    source_of, receiver = lengths[1:1 + 2 * pairs:2], lengths[2:2 + 2 * pairs:2]
    room = jnp.minimum(source_of - 1, most - receiver)
    shifted = jax.random.randint(jax.random.fold_in(stream_key, 1), (pairs,), 0, 1 << 20) % (room + 1)
    lengths = lengths.at[1:1 + 2 * pairs:2].set(source_of - shifted).at[2:2 + 2 * pairs:2].set(receiver + shifted)
    return lengths[jax.random.permutation(jax.random.fold_in(stream_key, 2), number_of)]


def setup_inputs(seed: int = 0) -> dict:
    streams_of = jax.random.split(jax.random.key(seed), 6)
    departures = draw_departures(jax.random.fold_in(streams_of[5], 71), 0)
    predictors = draw_predictors(jax.random.fold_in(streams_of[5], 71), 0)
    inv_band = draw_inv_band(jax.random.fold_in(streams_of[5], 71), 0)
    band_id = jnp.searchsorted(jnp.cumsum(ragged(streams_of[3], C // 24, C, MAXB, 1)), jnp.arange(C), side="right").astype(jnp.int32)
    line_counts = set_ends(jax.random.randint(streams_of[4], (LINES,), 24, LINE_SLOTS + 1), jax.random.fold_in(streams_of[4], 1), 24, LINE_SLOTS).astype(jnp.int32)
    return {"departures": departures, "predictors": predictors, "inv_band": inv_band, "band_id": band_id, "line_counts": line_counts}


huber_edge = 1.0


def reference(departures, predictors, inv_band, band_id, line_counts):
    chans, nobs = departures.shape
    half = MAXB - 1
    tile = 128
    extent = tile + 2 * half
    slots = jnp.arange(nobs, dtype=jnp.int32)
    live = (slots % LINE_SLOTS < jnp.repeat(line_counts, LINE_SLOTS)).astype(jnp.float32)
    pred_wide = predictors.astype(jnp.float32).T
    pairs_t = (pred_wide[:, :, None] * pred_wide[:, None, :]).reshape(nobs, P_SIZE * P_SIZE).astype(jnp.bfloat16)
    pred_t = predictors.T

    def one_tile(index):
        first = index * tile
        start = jnp.clip(first - half, 0, chans - extent).astype(jnp.int32)
        rows_at = first + jnp.arange(tile, dtype=jnp.int32)
        cols_at = start + jnp.arange(extent, dtype=jnp.int32)
        offset = cols_at[None, :] - rows_at[:, None] + half
        keep = (offset >= 0) & (offset <= 2 * half) & (band_id[cols_at][None, :] == band_id[rows_at][:, None])
        values = inv_band[jnp.clip(offset, 0, 2 * half), rows_at[:, None]]
        matrix = jnp.where(keep, values, jnp.zeros_like(values))
        window = lax.dynamic_slice_in_dim(departures, start, extent, 0)
        weighted = jnp.dot(matrix, window, preferred_element_type=jnp.float32)
        ratio = live[None, :] * (huber_edge / jnp.maximum(jnp.abs(weighted), huber_edge))
        qc_weight = ratio.astype(jnp.bfloat16)
        scaled = (ratio * weighted).astype(jnp.bfloat16)
        gram_tile = jnp.dot(qc_weight, pairs_t, preferred_element_type=jnp.float32)
        rhs_tile = jnp.dot(scaled, pred_t, preferred_element_type=jnp.float32)
        return gram_tile, rhs_tile

    grams, rhss = lax.map(one_tile, jnp.arange(chans // tile, dtype=jnp.int32))
    gram = grams.reshape(chans, P_SIZE * P_SIZE).T / jnp.float32(nobs)
    rhs = rhss.reshape(chans, P_SIZE).T / jnp.float32(nobs)
    return gram, rhs
```

```python
import functools

import jax
import jax.numpy as jnp
import numpy as np
from jax import lax
from jax.experimental import pallas as pl
from jax.experimental.pallas import tpu as pltpu
from jax.sharding import PartitionSpec as P

huber_edge = 1.0
LANES = 128
HALO = 32
TILE = 128
OBS_CHUNK = 512
MESH = pl.DeviceIdType.MESH


def mirror_rows(count):
    rows = []
    for first in range(count):
        for second in range(count):
            low = min(first, second)
            high = max(first, second)
            rows.append(low * count - low * (low - 1) // 2 + high - low)
    return rows


def peer(axis, index):
    if axis == "obs":
        return (index, lax.axis_index("chan"))
    return (lax.axis_index("obs"), index)


def kernel(
    n_obs,
    n_chan,
    scatter,
    dep,
    pred,
    inv,
    ids_win,
    ids_own,
    counts,
    *rest,
):
    if scatter:
        gram_out, rhs_out = rest[:2]
        rest = rest[2:]
    else:
        part_out = rest[0]
        rest = rest[1:]
    (
        window,
        wide,
        table_q,
        table_s,
        flip,
        stage,
        landed,
        total,
        load_sem,
        halo_send,
        halo_recv,
        part_send,
        part_recv,
    ) = rest
    own, obs_dev = dep.shape
    preds = pred.shape[0]
    offsets = inv.shape[0]
    half = offsets // 2
    upper = preds * (preds + 1) // 2
    rows = stage.shape[1]
    blocks = stage.shape[0]
    width = own // blocks
    lines = counts.shape[0]
    slots = obs_dev // lines
    me = lax.axis_index("obs")
    chan = lax.axis_index("chan")
    right = lax.rem(chan + 1, n_chan)
    left = lax.rem(chan + n_chan - 1, n_chan)

    barrier = pltpu.get_barrier_semaphore()
    for index in (left, right):
        pl.semaphore_signal(barrier, inc=1, device_id=peer("chan", index), device_id_type=MESH)
    greeted = 2
    if scatter:
        for step in range(1, n_obs):
            index = lax.rem(me + step, n_obs)
            pl.semaphore_signal(barrier, inc=1, device_id=peer("obs", index), device_id_type=MESH)
        greeted += n_obs - 1

    here = lax.rem(me, blocks)
    stride = jnp.where(here < blocks // 2, 1, blocks - 1)

    def block_at(place):
        return lax.rem(here + stride * place, blocks)

    def load(place):
        start = pl.multiple_of(block_at(place) * width, width)
        return pltpu.make_async_copy(
            dep.at[pl.ds(start, width), :],
            window.at[pl.ds(start + HALO, width), :],
            load_sem.at[place],
        )

    def start_load(place, carry):
        load(place).start()
        return carry

    lax.fori_loop(0, blocks, start_load, 0)

    values = pred[...].astype(jnp.float32)
    wide[...] = jnp.zeros_like(wide)
    first_row = 0
    for first in range(preds):
        count = preds - first
        wide[first_row : first_row + count, :] = values[first:, :] * values[first : first + 1, :]
        first_row += count
    wide[upper : upper + preds, :] = values
    lane = lax.broadcasted_iota(jnp.int32, (slots, LANES), 1)

    def turn(line, carry):
        at = pl.ds(pl.multiple_of(line * slots, slots), slots)
        slot = lax.broadcasted_iota(jnp.int32, (LANES, slots), 1)
        live = jnp.where(slot < counts[line], wide[:, at], 0.0)
        turned = live.T
        table_q[at, :] = jnp.where(lane < upper, turned, 0.0).astype(jnp.bfloat16)
        table_s[at, :] = jnp.where(lane >= upper, turned, 0.0).astype(jnp.bfloat16)
        return carry

    lax.fori_loop(0, lines, turn, 0)
    flip[...] = jnp.zeros_like(flip)

    pl.semaphore_wait(barrier, greeted)
    to_left = pltpu.make_async_remote_copy(
        src_ref=dep.at[pl.ds(0, HALO), :],
        dst_ref=window.at[pl.ds(own + HALO, HALO), :],
        send_sem=halo_send.at[0],
        recv_sem=halo_recv.at[0],
        device_id=peer("chan", left),
        device_id_type=MESH,
    )
    to_right = pltpu.make_async_remote_copy(
        src_ref=dep.at[pl.ds(own - HALO, HALO), :],
        dst_ref=window.at[pl.ds(0, HALO), :],
        send_sem=halo_send.at[1],
        recv_sem=halo_recv.at[1],
        device_id=peer("chan", right),
        device_id_type=MESH,
    )
    to_left.start()
    to_right.start()

    def send_part(step):
        return pltpu.make_async_remote_copy(
            src_ref=stage.at[step],
            dst_ref=landed.at[me],
            send_sem=part_send.at[step],
            recv_sem=part_recv.at[me],
            device_id=peer("obs", block_at(step + 1)),
            device_id_type=MESH,
        )

    def arrived(sender):
        return pltpu.make_async_remote_copy(
            src_ref=stage.at[0],
            dst_ref=landed.at[sender],
            send_sem=part_send.at[0],
            recv_sem=part_recv.at[sender],
            device_id=peer("obs", sender),
            device_id_type=MESH,
        )

    load(0).wait()
    load(1).wait()

    def one_block(step, carry):
        block = block_at(step + 1)

        @pl.when(step + 2 < blocks)
        def _():
            load(step + 2).wait()

        @pl.when(block == blocks - 1)
        def _():
            to_left.wait_recv()

        @pl.when(block == 0)
        def _():
            to_right.wait_recv()

        for part in range(width // TILE):
            first = pl.multiple_of(block * width + part * TILE, TILE)
            flip[0:offsets, :] = inv[:, pl.ds(first, TILE)].astype(jnp.float32)
            flip[64:65, :] = ids_own[:, pl.ds(first, TILE)]
            turned = flip[...].T
            own_id = turned[:, 64:65]
            place = lax.broadcasted_iota(jnp.int32, turned.shape, 1)
            turned = jnp.where(place < offsets, turned, 0.0)
            skewed = pltpu.roll(
                jnp.concatenate([turned, jnp.zeros_like(turned)], axis=1),
                HALO - half,
                1,
                stride=1,
                stride_axis=0,
            )
            same = ids_win[:, pl.ds(first, 2 * TILE)] == own_id
            matrix = jnp.where(same, skewed, 0.0).astype(jnp.bfloat16)
            matrix = matrix[:, : TILE + 2 * HALO]
            sums = jnp.zeros((TILE, LANES), jnp.float32)
            for at in range(0, obs_dev, OBS_CHUNK):
                weighted = jnp.dot(
                    matrix,
                    window[pl.ds(first, TILE + 2 * HALO), at : at + OBS_CHUNK],
                    preferred_element_type=jnp.float32,
                )
                ratio = huber_edge / jnp.maximum(jnp.abs(weighted), huber_edge)
                qc_weight = ratio.astype(jnp.bfloat16)
                scaled = jnp.clip(weighted, -huber_edge, huber_edge).astype(jnp.bfloat16)
                sums += jnp.dot(
                    qc_weight,
                    table_q[at : at + OBS_CHUNK, :],
                    preferred_element_type=jnp.float32,
                )
                sums += jnp.dot(
                    scaled,
                    table_s[at : at + OBS_CHUNK, :],
                    preferred_element_type=jnp.float32,
                )
            result = sums.T[:rows, :]
            if scatter:
                stage[step, :, part * TILE : (part + 1) * TILE] = result
            else:
                part_out[:, pl.ds(first, TILE)] = result

        if scatter:

            @pl.when(step < blocks - 1)
            def _():
                send_part(step).start()

        return carry

    lax.fori_loop(0, blocks, one_block, 0)
    to_left.wait_send()
    to_right.wait_send()

    if scatter:
        total[...] = stage[blocks - 1]

        def gather(step, carry):
            sender = block_at(blocks - step)
            arrived(sender).wait_recv()
            total[...] += landed[sender]
            return carry

        lax.fori_loop(1, blocks, gather, 0)
        factor = 1.0 / float(obs_dev * n_obs)
        total[...] = total[...] * factor
        for row, source in enumerate(mirror_rows(preds)):
            gram_out[row : row + 1, :] = total[source : source + 1, :]
        rhs_out[...] = total[upper : upper + preds, :]

        def drain(step, carry):
            send_part(step).wait_send()
            return carry

        lax.fori_loop(0, blocks - 1, drain, 0)


def on_device(departures, predictors, inv_band, band_id, line_counts):
    own, obs_dev = departures.shape
    preds = predictors.shape[0]
    upper = preds * (preds + 1) // 2
    n_obs = lax.axis_size("obs")
    n_chan = lax.axis_size("chan")
    share = own // n_obs
    scatter = share % TILE == 0
    blocks = n_obs if scatter else own // (2 * TILE)
    width = own // blocks
    rows = -(-(upper + preds) // 8) * 8
    base = lax.axis_index("chan") * own
    marked = jnp.pad(band_id, (HALO, TILE), constant_values=-1).astype(jnp.float32)
    ids_win = lax.dynamic_slice_in_dim(marked, base, own + TILE)[None, :]
    ids_own = lax.dynamic_slice_in_dim(marked, base + HALO, own)[None, :]
    if scatter:
        out_shape = (
            jax.ShapeDtypeStruct((preds * preds, share), jnp.float32),
            jax.ShapeDtypeStruct((preds, share), jnp.float32),
        )
    else:
        out_shape = (jax.ShapeDtypeStruct((rows, own), jnp.float32),)
    vmem = pl.BlockSpec(memory_space=pltpu.VMEM)
    landing = (n_obs, rows, width) if scatter else (1, 8, LANES)
    outs = pl.pallas_call(
        functools.partial(kernel, n_obs, n_chan, scatter),
        out_shape=out_shape,
        in_specs=[
            pl.BlockSpec(memory_space=pl.ANY),
            vmem,
            vmem,
            vmem,
            vmem,
            pl.BlockSpec(memory_space=pltpu.SMEM),
        ],
        out_specs=tuple(vmem for _ in out_shape),
        scratch_shapes=[
            pltpu.VMEM((own + 2 * HALO, obs_dev), jnp.bfloat16),
            pltpu.VMEM((LANES, obs_dev), jnp.float32),
            pltpu.VMEM((obs_dev, LANES), jnp.bfloat16),
            pltpu.VMEM((obs_dev, LANES), jnp.bfloat16),
            pltpu.VMEM((LANES, TILE), jnp.float32),
            pltpu.VMEM((blocks, rows, width), jnp.float32),
            pltpu.VMEM(landing, jnp.float32),
            pltpu.VMEM((rows, width), jnp.float32),
            pltpu.SemaphoreType.DMA((blocks,)),
            pltpu.SemaphoreType.DMA((2,)),
            pltpu.SemaphoreType.DMA((2,)),
            pltpu.SemaphoreType.DMA((blocks,)),
            pltpu.SemaphoreType.DMA((n_obs,)),
        ],
        compiler_params=pltpu.CompilerParams(
            collective_id=0,
            has_side_effects=True,
            vmem_limit_bytes=40 * 1024 * 1024,
        ),
        name="normal_equations",
    )(departures, predictors, inv_band, ids_win, ids_own, line_counts)
    if scatter:
        return outs[0], outs[1]
    factor = 1.0 / float(obs_dev * n_obs)
    part = lax.psum_scatter(outs[0], "obs", scatter_dimension=1, tiled=True) * factor
    mirror = np.array(mirror_rows(preds))
    return part[mirror], part[upper : upper + preds]


def solution(mesh):
    in_specs = (P("chan", "obs"), P(None, "obs"), P(None, "chan"), P(), P("obs"))
    out_specs = (P(None, ("chan", "obs")), P(None, ("chan", "obs")))
    return jax.shard_map(
        on_device, mesh=mesh, in_specs=in_specs, out_specs=out_specs, check_vma=False
    )
```

```python
import functools

import jax
import jax.numpy as jnp
import numpy as np
from jax import lax
from jax.experimental import pallas as pl
from jax.experimental.pallas import tpu as pltpu
from jax.sharding import PartitionSpec as P

huber_edge = 1.0
LANES = 128
HALO = 32
TILE = 128
OBS_CHUNK = 512
MESH = pl.DeviceIdType.MESH


def mirror_rows(count):
    rows = []
    for first in range(count):
        for second in range(count):
            low = min(first, second)
            high = max(first, second)
            rows.append(low * count - low * (low - 1) // 2 + high - low)
    return rows


def peer(axis, index):
    if axis == "obs":
        return (index, lax.axis_index("chan"))
    return (lax.axis_index("obs"), index)


def kernel(n_obs, n_chan, scatter, dep, pred, inv, ids, counts, *rest):
    if scatter:
        gram_out, rhs_out = rest[:2]
        rest = rest[2:]
    else:
        part_out = rest[0]
        rest = rest[1:]
    (
        window,
        pred_in,
        inv_in,
        ids_in,
        counts_in,
        wide,
        table,
        flip,
        bands,
        stage,
        landed_x,
        landed_z,
        total,
        small_sem,
        load_sem,
        halo_send,
        halo_recv,
        x_send,
        x_recv,
        z_send,
        z_recv,
    ) = rest
    own, obs_dev = dep.shape
    preds = pred.shape[0]
    offsets = inv.shape[0]
    half = offsets // 2
    upper = preds * (preds + 1) // 2
    blocks, rows, width = stage.shape
    tiles = width // TILE
    pairs = blocks // 2
    lines = counts.shape[0]
    slots = obs_dev // lines
    me = lax.axis_index("obs")
    chan = lax.axis_index("chan")
    right = lax.rem(chan + 1, n_chan)
    left = lax.rem(chan + n_chan - 1, n_chan)
    spot = lax.rem(me, blocks)
    col = lax.rem(spot, 2)
    lev = lax.div(spot, 2)
    stride = jnp.where(lev < pairs // 2, 1, pairs - 1)

    def level_at(turn):
        return lax.rem(lev + stride * (turn + 1), pairs)

    def block_at(step):
        side = jnp.where(step < pairs, 1 - col, col)
        return 2 * level_at(lax.rem(step, pairs)) + side

    barrier = pltpu.get_barrier_semaphore()
    for index in (left, right):
        pl.semaphore_signal(barrier, inc=1, device_id=peer("chan", index), device_id_type=MESH)
    greeted = 2
    if scatter:
        partner = me + 1 - 2 * col
        pl.semaphore_signal(barrier, inc=1, device_id=peer("obs", partner), device_id_type=MESH)
        for turn in range(pairs - 1):
            index = 2 * level_at(turn) + col
            pl.semaphore_signal(barrier, inc=1, device_id=peer("obs", index), device_id_type=MESH)
        greeted += pairs

    base = pl.multiple_of(chan * own, own)
    smalls = [
        pltpu.make_async_copy(pred, pred_in, small_sem.at[0]),
        pltpu.make_async_copy(counts, counts_in, small_sem.at[1]),
        pltpu.make_async_copy(inv, inv_in, small_sem.at[2]),
        pltpu.make_async_copy(
            ids.at[:, pl.ds(base, own)], ids_in.at[:, pl.ds(LANES, own)], small_sem.at[3]
        ),
    ]
    before = pltpu.make_async_copy(
        ids.at[:, pl.ds(pl.multiple_of(jnp.maximum(base - LANES, 0), LANES), LANES)],
        ids_in.at[:, pl.ds(0, LANES)],
        small_sem.at[4],
    )
    after = pltpu.make_async_copy(
        ids.at[:, pl.ds(pl.multiple_of(jnp.minimum(base + own, own * n_chan - LANES), LANES), LANES)],
        ids_in.at[:, pl.ds(LANES + own, LANES)],
        small_sem.at[5],
    )
    for copy in smalls:
        copy.start()
    before.start()
    after.start()

    origin = block_at(0) + blocks - jnp.where(stride == 1, 1, blocks - 1)
    hop = jnp.where(stride == 1, 1, blocks - 1)

    def load(place):
        chunk = lax.rem(origin + hop * place, blocks)
        start = pl.multiple_of(chunk * width, width)
        return pltpu.make_async_copy(
            dep.at[pl.ds(start, width), :],
            window.at[pl.ds(start + HALO, width), :],
            load_sem.at[place],
        )

    def start_load(place, carry):
        load(place).start()
        return carry

    lax.fori_loop(0, blocks, start_load, 0)

    smalls[0].wait()
    smalls[1].wait()
    values = pred_in[...].astype(jnp.float32)
    wide[upper + preds :, :] = jnp.zeros((LANES - upper - preds, obs_dev), jnp.float32)
    first_row = 0
    for first in range(preds):
        count = preds - first
        wide[first_row : first_row + count, :] = values[first:, :] * values[first : first + 1, :]
        first_row += count
    wide[upper : upper + preds, :] = values
    lane = lax.broadcasted_iota(jnp.int32, (slots, LANES), 1)

    def turn_line(line, carry):
        at = pl.ds(pl.multiple_of(line * slots, slots), slots)
        slot = lax.broadcasted_iota(jnp.int32, (LANES, slots), 1)
        live = jnp.where(slot < counts_in[line], wide[:, at], 0.0)
        turned = live.T
        per = OBS_CHUNK // slots
        spot_q = pl.multiple_of(lax.div(line, per) * 2 * OBS_CHUNK + lax.rem(line, per) * slots, slots)
        table[pl.ds(spot_q, slots), :] = jnp.where(lane < upper, turned, 0.0).astype(jnp.bfloat16)
        table[pl.ds(spot_q + OBS_CHUNK, slots), :] = jnp.where(lane >= upper, turned, 0.0).astype(
            jnp.bfloat16
        )
        return carry

    lax.fori_loop(0, lines, turn_line, 0, unroll=2)

    pl.semaphore_wait(barrier, greeted)
    to_left = pltpu.make_async_remote_copy(
        src_ref=dep.at[pl.ds(0, HALO), :],
        dst_ref=window.at[pl.ds(own + HALO, HALO), :],
        send_sem=halo_send.at[0],
        recv_sem=halo_recv.at[0],
        device_id=peer("chan", left),
        device_id_type=MESH,
    )
    to_right = pltpu.make_async_remote_copy(
        src_ref=dep.at[pl.ds(own - HALO, HALO), :],
        dst_ref=window.at[pl.ds(0, HALO), :],
        send_sem=halo_send.at[1],
        recv_sem=halo_recv.at[1],
        device_id=peer("chan", right),
        device_id_type=MESH,
    )
    to_left.start()
    to_right.start()

    smalls[2].wait()
    smalls[3].wait()
    before.wait()
    after.wait()

    @pl.when(chan == 0)
    def _():
        ids_in[:, 0:LANES] = jnp.full((1, LANES), -1, jnp.int32)

    @pl.when(chan == n_chan - 1)
    def _():
        ids_in[:, LANES + own :] = jnp.full((1, LANES), -1, jnp.int32)

    flip[...] = jnp.zeros_like(flip)

    def build(group, carry):
        for lane_of in range(flip.shape[0]):
            first = pl.multiple_of((group * flip.shape[0] + lane_of) * TILE, TILE)
            near = ids_in[:, pl.ds(first, 3 * TILE)].astype(jnp.float32)
            flip[lane_of, 0:offsets, :] = inv_in[:, pl.ds(first, TILE)].astype(jnp.float32)
            flip[lane_of, 64:65, :] = near[:, TILE : 2 * TILE]
            turned = flip[lane_of].T
            own_id = turned[:, 64:65]
            place = lax.broadcasted_iota(jnp.int32, turned.shape, 1)
            turned = jnp.where(place < offsets, turned, 0.0)
            skewed = pltpu.roll(
                jnp.concatenate([turned, jnp.zeros_like(turned)], axis=1),
                HALO - half,
                1,
                stride=1,
                stride_axis=0,
            )
            same = near[:, TILE - HALO : 3 * TILE - HALO] == own_id
            bands[pl.ds(first, TILE), :] = jnp.where(same, skewed, 0.0).astype(jnp.bfloat16)
        return carry

    lax.fori_loop(0, own // TILE // flip.shape[0], build, 0)

    def send_x(turn):
        return pltpu.make_async_remote_copy(
            src_ref=stage.at[turn],
            dst_ref=landed_x.at[turn],
            send_sem=x_send.at[turn],
            recv_sem=x_recv.at[turn],
            device_id=peer("obs", partner),
            device_id_type=MESH,
        )

    def send_z(turn):
        return pltpu.make_async_remote_copy(
            src_ref=stage.at[pairs + turn],
            dst_ref=landed_z.at[lev],
            send_sem=z_send.at[turn],
            recv_sem=z_recv.at[lev],
            device_id=peer("obs", 2 * level_at(turn) + col),
            device_id_type=MESH,
        )

    def from_z(turn):
        sender = level_at(turn)
        return pltpu.make_async_remote_copy(
            src_ref=stage.at[pairs],
            dst_ref=landed_z.at[sender],
            send_sem=z_send.at[0],
            recv_sem=z_recv.at[sender],
            device_id=peer("obs", 2 * sender + col),
            device_id_type=MESH,
        )

    load(0).wait()

    def one_block(step, carry):
        block = block_at(step)

        @pl.when(step < pairs)
        def _():
            load(2 * step + 1).wait()

        @pl.when(step < pairs - 1)
        def _():
            load(2 * step + 2).wait()

        @pl.when(block == blocks - 1)
        def _():
            to_left.wait_recv()

        @pl.when(block == 0)
        def _():
            to_right.wait_recv()

        start = pl.multiple_of(block * width, width)
        extent = TILE + 2 * HALO
        sums = jnp.zeros((width, LANES), jnp.float32)
        for at in range(0, obs_dev, OBS_CHUNK):
            parts = []
            for part in range(tiles):
                first = pl.multiple_of(start + part * TILE, TILE)
                weighted = jnp.dot(
                    bands[pl.ds(first, TILE), 0:extent],
                    window[pl.ds(first, extent), at : at + OBS_CHUNK],
                    preferred_element_type=jnp.float32,
                )
                ratio = huber_edge / jnp.maximum(jnp.abs(weighted), huber_edge)
                qc_weight = ratio.astype(jnp.bfloat16)
                scaled = jnp.clip(weighted, -huber_edge, huber_edge).astype(jnp.bfloat16)
                parts.append(jnp.concatenate([qc_weight, scaled], axis=1))
            sums += jnp.dot(
                jnp.concatenate(parts, axis=0),
                table[2 * at : 2 * (at + OBS_CHUNK), :],
                preferred_element_type=jnp.float32,
            )
        result = sums.T[:rows, :]
        if not scatter:
            part_out[:, pl.ds(start, width)] = result
            return carry
        turn = lax.rem(step, pairs)

        @pl.when(step < pairs)
        def _():
            stage[step] = result
            send_x(turn).start()

        @pl.when(step >= pairs)
        def _():
            send_x(turn).wait_recv()
            stage[step] = result + landed_x[turn]

            @pl.when(step < blocks - 1)
            def _():
                send_z(turn).start()

        return carry

    lax.fori_loop(0, blocks, one_block, 0)
    to_left.wait_send()
    to_right.wait_send()

    if scatter:
        sums = stage[blocks - 1]
        for turn in range(pairs - 2, -1, -1):
            from_z(turn).wait_recv()
            sums = sums + landed_z[level_at(turn)]
        total[...] = sums * (1.0 / float(obs_dev * n_obs))
        for row, source in enumerate(mirror_rows(preds)):
            gram_out[row : row + 1, :] = total[source : source + 1, :]
        rhs_out[...] = total[upper : upper + preds, :]
        for turn in range(pairs):
            send_x(turn).wait_send()
        for turn in range(pairs - 1):
            send_z(turn).wait_send()


def on_device(departures, predictors, inv_band, band_id, line_counts):
    own, obs_dev = departures.shape
    preds = predictors.shape[0]
    upper = preds * (preds + 1) // 2
    n_obs = lax.axis_size("obs")
    n_chan = lax.axis_size("chan")
    share = own // n_obs
    scatter = share % TILE == 0 and n_obs % 2 == 0
    blocks = n_obs if scatter else own // (2 * TILE)
    width = own // blocks
    rows = -(-(upper + preds) // 8) * 8
    if scatter:
        out_shape = (
            jax.ShapeDtypeStruct((preds * preds, share), jnp.float32),
            jax.ShapeDtypeStruct((preds, share), jnp.float32),
        )
    else:
        out_shape = (jax.ShapeDtypeStruct((rows, own), jnp.float32),)
    vmem = pl.BlockSpec(memory_space=pltpu.VMEM)
    hbm = pl.BlockSpec(memory_space=pltpu.HBM)
    pairs = blocks // 2
    landing = (pairs, rows, width) if scatter else (1, 8, LANES)
    dma = pltpu.SemaphoreType.DMA
    outs = pl.pallas_call(
        functools.partial(kernel, n_obs, n_chan, scatter),
        out_shape=out_shape,
        in_specs=[hbm] * 5,
        out_specs=tuple(vmem for _ in out_shape),
        scratch_shapes=[
            pltpu.VMEM((own + 2 * HALO, obs_dev), jnp.bfloat16),
            pltpu.VMEM(predictors.shape, jnp.bfloat16),
            pltpu.VMEM(inv_band.shape, jnp.bfloat16),
            pltpu.VMEM((1, own + 2 * LANES), jnp.int32),
            pltpu.SMEM(line_counts.shape, jnp.int32),
            pltpu.VMEM((LANES, obs_dev), jnp.float32),
            pltpu.VMEM((2 * obs_dev, LANES), jnp.bfloat16),
            pltpu.VMEM((4, LANES, TILE), jnp.float32),
            pltpu.VMEM((own, 2 * TILE), jnp.bfloat16),
            pltpu.VMEM((blocks, rows, width), jnp.float32),
            pltpu.VMEM(landing, jnp.float32),
            pltpu.VMEM(landing, jnp.float32),
            pltpu.VMEM((rows, width), jnp.float32),
            dma((6,)),
            dma((blocks,)),
            dma((2,)),
            dma((2,)),
            dma((pairs,)),
            dma((pairs,)),
            dma((pairs,)),
            dma((pairs,)),
        ],
        compiler_params=pltpu.CompilerParams(
            collective_id=0,
            has_side_effects=True,
            vmem_limit_bytes=67043328,
        ),
        name="normal_equations",
    )(departures, predictors, inv_band, band_id[None, :], line_counts)
    if scatter:
        return outs[0], outs[1]
    factor = 1.0 / float(obs_dev * n_obs)
    part = lax.psum_scatter(outs[0], "obs", scatter_dimension=1, tiled=True) * factor
    mirror = np.array(mirror_rows(preds))
    return part[mirror], part[upper : upper + preds]


def solution(mesh):
    in_specs = (P("chan", "obs"), P(None, "obs"), P(None, "chan"), P(), P("obs"))
    out_specs = (P(None, ("chan", "obs")), P(None, ("chan", "obs")))
    return jax.shard_map(
        on_device, mesh=mesh, in_specs=in_specs, out_specs=out_specs, check_vma=False
    )
```

```python
import functools

import jax
import jax.numpy as jnp
import numpy as np
from jax import lax
from jax.experimental import pallas as pl
from jax.experimental.pallas import tpu as pltpu
from jax.sharding import PartitionSpec as P

huber_edge = 1.0
LANES = 128
HALO = 32
TILE = 128
OBS_CHUNK = 1024
MESH = pl.DeviceIdType.MESH


def mirror_rows(count):
    rows = []
    for first in range(count):
        for second in range(count):
            low = min(first, second)
            high = max(first, second)
            rows.append(low * count - low * (low - 1) // 2 + high - low)
    return rows


def peer(axis, index):
    if axis == "obs":
        return (index, lax.axis_index("chan"))
    return (lax.axis_index("obs"), index)


def kernel(n_obs, n_chan, scatter, dep, pred, inv, ids, counts, *rest):
    if scatter:
        gram_out, rhs_out = rest[:2]
        rest = rest[2:]
    else:
        part_out = rest[0]
        rest = rest[1:]
    (
        window,
        pred_in,
        inv_in,
        ids_in,
        counts_in,
        wide,
        table,
        flip,
        bands,
        stage,
        landed_x,
        landed_z,
        total,
        small_sem,
        load_sem,
        halo_send,
        halo_recv,
        x_send,
        x_recv,
        z_send,
        z_recv,
    ) = rest
    own, obs_dev = dep.shape
    preds = pred.shape[0]
    offsets = inv.shape[0]
    half = offsets // 2
    upper = preds * (preds + 1) // 2
    blocks, rows, width = stage.shape
    tiles = width // TILE
    pairs = blocks // 2
    lines = counts.shape[0]
    slots = obs_dev // lines
    me = lax.axis_index("obs")
    chan = lax.axis_index("chan")
    right = lax.rem(chan + 1, n_chan)
    left = lax.rem(chan + n_chan - 1, n_chan)
    spot = lax.rem(me, blocks)
    col = lax.rem(spot, 2)
    lev = lax.div(spot, 2)
    stride = jnp.where(lev < pairs // 2, 1, pairs - 1)

    def level_at(turn):
        return lax.rem(lev + stride * (turn + 1), pairs)

    def for_partner(step):
        odd = lax.rem(step, 2) == 1
        return jnp.logical_or(step == 0, jnp.logical_and(odd, step < blocks - 1))

    def turn_at(step):
        return jnp.where(for_partner(step), lax.div(step + 1, 2), lax.div(jnp.maximum(step - 1, 0), 2))

    def block_at(step):
        side = jnp.where(for_partner(step), 1 - col, col)
        return 2 * level_at(turn_at(step)) + side

    barrier = pltpu.get_barrier_semaphore()
    for index in (left, right):
        pl.semaphore_signal(barrier, inc=1, device_id=peer("chan", index), device_id_type=MESH)
    greeted = 2
    if scatter:
        partner = me + 1 - 2 * col
        pl.semaphore_signal(barrier, inc=1, device_id=peer("obs", partner), device_id_type=MESH)
        for turn in range(pairs - 1):
            index = 2 * level_at(turn) + col
            pl.semaphore_signal(barrier, inc=1, device_id=peer("obs", index), device_id_type=MESH)
        greeted += pairs

    base = pl.multiple_of(chan * own, own)
    smalls = [
        pltpu.make_async_copy(pred, pred_in, small_sem.at[0]),
        pltpu.make_async_copy(counts, counts_in, small_sem.at[1]),
        pltpu.make_async_copy(inv, inv_in, small_sem.at[2]),
        pltpu.make_async_copy(
            ids.at[:, pl.ds(base, own)], ids_in.at[:, pl.ds(LANES, own)], small_sem.at[3]
        ),
    ]
    before = pltpu.make_async_copy(
        ids.at[:, pl.ds(pl.multiple_of(jnp.maximum(base - LANES, 0), LANES), LANES)],
        ids_in.at[:, pl.ds(0, LANES)],
        small_sem.at[4],
    )
    after = pltpu.make_async_copy(
        ids.at[:, pl.ds(pl.multiple_of(jnp.minimum(base + own, own * n_chan - LANES), LANES), LANES)],
        ids_in.at[:, pl.ds(LANES + own, LANES)],
        small_sem.at[5],
    )
    for copy in smalls:
        copy.start()
    before.start()
    after.start()

    origin = block_at(0) + blocks - jnp.where(stride == 1, 1, blocks - 1)
    hop = jnp.where(stride == 1, 1, blocks - 1)

    def load(place):
        chunk = lax.rem(origin + hop * place, blocks)
        start = pl.multiple_of(chunk * width, width)
        return pltpu.make_async_copy(
            dep.at[pl.ds(start, width), :],
            window.at[pl.ds(start + HALO, width), :],
            load_sem.at[place],
        )

    def start_load(place, carry):
        load(place).start()
        return carry

    lax.fori_loop(0, blocks, start_load, 0)

    smalls[0].wait()
    smalls[1].wait()
    values = pred_in[...].astype(jnp.float32)
    wide[upper + preds :, :] = jnp.zeros((LANES - upper - preds, obs_dev), jnp.float32)
    first_row = 0
    for first in range(preds):
        count = preds - first
        wide[first_row : first_row + count, :] = values[first:, :] * values[first : first + 1, :]
        first_row += count
    wide[upper : upper + preds, :] = values
    lane = lax.broadcasted_iota(jnp.int32, (slots, LANES), 1)

    def turn_line(line, carry):
        at = pl.ds(pl.multiple_of(line * slots, slots), slots)
        slot = lax.broadcasted_iota(jnp.int32, (LANES, slots), 1)
        live = jnp.where(slot < counts_in[line], wide[:, at], 0.0)
        turned = live.T
        per = OBS_CHUNK // slots
        spot_q = pl.multiple_of(lax.div(line, per) * 2 * OBS_CHUNK + lax.rem(line, per) * slots, slots)
        table[pl.ds(spot_q, slots), :] = jnp.where(lane < upper, turned, 0.0).astype(jnp.bfloat16)
        table[pl.ds(spot_q + OBS_CHUNK, slots), :] = jnp.where(lane >= upper, turned, 0.0).astype(
            jnp.bfloat16
        )
        return carry

    lax.fori_loop(0, lines, turn_line, 0, unroll=2)

    pl.semaphore_wait(barrier, greeted)
    to_left = pltpu.make_async_remote_copy(
        src_ref=dep.at[pl.ds(0, HALO), :],
        dst_ref=window.at[pl.ds(own + HALO, HALO), :],
        send_sem=halo_send.at[0],
        recv_sem=halo_recv.at[0],
        device_id=peer("chan", left),
        device_id_type=MESH,
    )
    to_right = pltpu.make_async_remote_copy(
        src_ref=dep.at[pl.ds(own - HALO, HALO), :],
        dst_ref=window.at[pl.ds(0, HALO), :],
        send_sem=halo_send.at[1],
        recv_sem=halo_recv.at[1],
        device_id=peer("chan", right),
        device_id_type=MESH,
    )
    to_left.start()
    to_right.start()

    smalls[2].wait()
    smalls[3].wait()
    before.wait()
    after.wait()

    @pl.when(chan == 0)
    def _():
        ids_in[:, 0:LANES] = jnp.full((1, LANES), -1, jnp.int32)

    @pl.when(chan == n_chan - 1)
    def _():
        ids_in[:, LANES + own :] = jnp.full((1, LANES), -1, jnp.int32)

    flip[...] = jnp.zeros_like(flip)

    def build(block):
        for part in range(tiles):
            first = pl.multiple_of(block * width + part * TILE, TILE)
            near = ids_in[:, pl.ds(first, 3 * TILE)].astype(jnp.float32)
            flip[part, 0:offsets, :] = inv_in[:, pl.ds(first, TILE)].astype(jnp.float32)
            flip[part, 64:65, :] = near[:, TILE : 2 * TILE]
            turned = flip[part].T
            own_id = turned[:, 64:65]
            place = lax.broadcasted_iota(jnp.int32, turned.shape, 1)
            turned = jnp.where(place < offsets, turned, 0.0)
            skewed = pltpu.roll(
                jnp.concatenate([turned, jnp.zeros_like(turned)], axis=1),
                HALO - half,
                1,
                stride=1,
                stride_axis=0,
            )
            same = near[:, TILE - HALO : 3 * TILE - HALO] == own_id
            bands[part * TILE : (part + 1) * TILE, :] = jnp.where(same, skewed, 0.0).astype(
                jnp.bfloat16
            )

    def send_x(turn):
        return pltpu.make_async_remote_copy(
            src_ref=stage.at[turn],
            dst_ref=landed_x.at[turn],
            send_sem=x_send.at[turn],
            recv_sem=x_recv.at[turn],
            device_id=peer("obs", partner),
            device_id_type=MESH,
        )

    def send_z(turn):
        return pltpu.make_async_remote_copy(
            src_ref=stage.at[pairs + turn],
            dst_ref=landed_z.at[lev],
            send_sem=z_send.at[turn],
            recv_sem=z_recv.at[lev],
            device_id=peer("obs", 2 * level_at(turn) + col),
            device_id_type=MESH,
        )

    def from_z(turn):
        sender = level_at(turn)
        return pltpu.make_async_remote_copy(
            src_ref=stage.at[pairs],
            dst_ref=landed_z.at[sender],
            send_sem=z_send.at[0],
            recv_sem=z_recv.at[sender],
            device_id=peer("obs", 2 * sender + col),
            device_id_type=MESH,
        )

    for place in range(3):
        load(place).wait()
    build(block_at(0))

    def one_block(step, carry):
        block = block_at(step)

        @pl.when(step == 1)
        def _():
            for place in range(3, 5):
                load(place).wait()

        @pl.when(step == 2)
        def _():
            for place in range(5, blocks):
                load(place).wait()

        @pl.when(block == blocks - 1)
        def _():
            to_left.wait_recv()

        @pl.when(block == 0)
        def _():
            to_right.wait_recv()

        start = pl.multiple_of(block * width, width)
        extent = TILE + 2 * HALO
        sums = jnp.zeros((width, LANES), jnp.float32)
        matrices = [bands[part * TILE : (part + 1) * TILE, 0:extent] for part in range(tiles)]
        for at in range(0, obs_dev, OBS_CHUNK):
            parts = []
            for part in range(tiles):
                first = pl.multiple_of(start + part * TILE, TILE)
                weighted = jnp.dot(
                    matrices[part],
                    window[pl.ds(first, extent), at : at + OBS_CHUNK],
                    preferred_element_type=jnp.float32,
                )
                ratio = huber_edge / jnp.maximum(jnp.abs(weighted), huber_edge)
                qc_weight = ratio.astype(jnp.bfloat16)
                scaled = jnp.clip(weighted, -huber_edge, huber_edge).astype(jnp.bfloat16)
                parts.append(jnp.concatenate([qc_weight, scaled], axis=1))
            sums += jnp.dot(
                jnp.concatenate(parts, axis=0),
                table[2 * at : 2 * (at + OBS_CHUNK), :],
                preferred_element_type=jnp.float32,
            )
        build(block_at(jnp.minimum(step + 1, blocks - 1)))
        result = sums.T[:rows, :]
        if not scatter:
            part_out[:, pl.ds(start, width)] = result
            return carry
        turn = turn_at(step)

        @pl.when(for_partner(step))
        def _():
            stage[turn] = result
            send_x(turn).start()

        @pl.when(jnp.logical_not(for_partner(step)))
        def _():
            send_x(turn).wait_recv()
            stage[pairs + turn] = result + landed_x[turn]

            @pl.when(step < blocks - 1)
            def _():
                send_z(turn).start()

        return carry

    lax.fori_loop(0, blocks, one_block, 0)
    to_left.wait_send()
    to_right.wait_send()

    if scatter:
        sums = stage[blocks - 1]
        for turn in range(pairs - 2, -1, -1):
            from_z(turn).wait_recv()
            sums = sums + landed_z[level_at(turn)]
        total[...] = sums * (1.0 / float(obs_dev * n_obs))
        for row, source in enumerate(mirror_rows(preds)):
            gram_out[row : row + 1, :] = total[source : source + 1, :]
        rhs_out[...] = total[upper : upper + preds, :]
        for turn in range(pairs):
            send_x(turn).wait_send()
        for turn in range(pairs - 1):
            send_z(turn).wait_send()


def on_device(departures, predictors, inv_band, band_id, line_counts):
    own, obs_dev = departures.shape
    preds = predictors.shape[0]
    upper = preds * (preds + 1) // 2
    n_obs = lax.axis_size("obs")
    n_chan = lax.axis_size("chan")
    share = own // n_obs
    scatter = share % TILE == 0 and n_obs % 2 == 0
    blocks = n_obs if scatter else own // (2 * TILE)
    width = own // blocks
    rows = -(-(upper + preds) // 8) * 8
    if scatter:
        out_shape = (
            pltpu.VMEM((preds * preds, share), jnp.float32),
            pltpu.VMEM((preds, share), jnp.float32),
        )
    else:
        out_shape = (jax.ShapeDtypeStruct((rows, own), jnp.float32),)
    vmem = pl.BlockSpec(memory_space=pltpu.VMEM)
    hbm = pl.BlockSpec(memory_space=pltpu.HBM)
    pairs = blocks // 2
    landing = (pairs, rows, width) if scatter else (1, 8, LANES)
    dma = pltpu.SemaphoreType.DMA
    outs = pl.pallas_call(
        functools.partial(kernel, n_obs, n_chan, scatter),
        out_shape=out_shape,
        in_specs=[hbm] * 5,
        out_specs=tuple(vmem for _ in out_shape),
        scratch_shapes=[
            pltpu.VMEM((own + 2 * HALO, obs_dev), jnp.bfloat16),
            pltpu.VMEM(predictors.shape, jnp.bfloat16),
            pltpu.VMEM(inv_band.shape, jnp.bfloat16),
            pltpu.VMEM((1, own + 2 * LANES), jnp.int32),
            pltpu.SMEM(line_counts.shape, jnp.int32),
            pltpu.VMEM((LANES, obs_dev), jnp.float32),
            pltpu.VMEM((2 * obs_dev, LANES), jnp.bfloat16),
            pltpu.VMEM((width // TILE, LANES, TILE), jnp.float32),
            pltpu.VMEM((width, 2 * TILE), jnp.bfloat16),
            pltpu.VMEM((blocks, rows, width), jnp.float32),
            pltpu.VMEM(landing, jnp.float32),
            pltpu.VMEM(landing, jnp.float32),
            pltpu.VMEM((rows, width), jnp.float32),
            dma((6,)),
            dma((blocks,)),
            dma((2,)),
            dma((2,)),
            dma((pairs,)),
            dma((pairs,)),
            dma((pairs,)),
            dma((pairs,)),
        ],
        compiler_params=pltpu.CompilerParams(
            collective_id=0,
            has_side_effects=True,
            vmem_limit_bytes=67043328 - 120 * 1024,
        ),
        name="normal_equations",
    )(departures, predictors, inv_band, band_id[None, :], line_counts)
    if scatter:
        return outs[0], outs[1]
    factor = 1.0 / float(obs_dev * n_obs)
    part = lax.psum_scatter(outs[0], "obs", scatter_dimension=1, tiled=True) * factor
    mirror = np.array(mirror_rows(preds))
    return part[mirror], part[upper : upper + preds]


def solution(mesh):
    in_specs = (P("chan", "obs"), P(None, "obs"), P(None, "chan"), P(), P("obs"))
    out_specs = (P(None, ("chan", "obs")), P(None, ("chan", "obs")))
    return jax.shard_map(
        on_device, mesh=mesh, in_specs=in_specs, out_specs=out_specs, check_vma=False
    )
```

```python
import functools

import jax
import jax.numpy as jnp
import numpy as np
from jax import lax
from jax.experimental import pallas as pl
from jax.experimental.pallas import tpu as pltpu
from jax.sharding import PartitionSpec as P

huber_edge = 1.0
LANES = 128
HALO = 32
TILE = 128
OBS_CHUNK = 2048
MESH = pl.DeviceIdType.MESH


def mirror_rows(count):
    rows = []
    for first in range(count):
        for second in range(count):
            low = min(first, second)
            high = max(first, second)
            rows.append(low * count - low * (low - 1) // 2 + high - low)
    return rows


def peer(axis, index):
    if axis == "obs":
        return (index, lax.axis_index("chan"))
    return (lax.axis_index("obs"), index)


def kernel(n_obs, n_chan, scatter, dep, pred, inv, ids, counts, *rest):
    if scatter:
        gram_out, rhs_out = rest[:2]
        rest = rest[2:]
    else:
        part_out = rest[0]
        rest = rest[1:]
    (
        window,
        pred_in,
        inv_in,
        ids_in,
        counts_in,
        wide,
        table,
        flip,
        bands,
        stage,
        landed_x,
        landed_z,
        total,
        small_sem,
        load_sem,
        halo_send,
        halo_recv,
        x_send,
        x_recv,
        z_send,
        z_recv,
    ) = rest
    own, obs_dev = dep.shape
    preds = pred.shape[0]
    offsets = inv.shape[0]
    half = offsets // 2
    upper = preds * (preds + 1) // 2
    blocks, rows, width = stage.shape
    tiles = width // TILE
    pairs = blocks // 2
    lines = counts.shape[0]
    slots = obs_dev // lines
    me = lax.axis_index("obs")
    chan = lax.axis_index("chan")
    right = lax.rem(chan + 1, n_chan)
    left = lax.rem(chan + n_chan - 1, n_chan)
    spot = lax.rem(me, blocks)
    col = lax.rem(spot, 2)
    lev = lax.div(spot, 2)
    stride = jnp.where(lev < pairs // 2, 1, pairs - 1)

    def level_at(turn):
        return lax.rem(lev + stride * (turn + 1), pairs)

    def for_partner(step):
        odd = lax.rem(step, 2) == 1
        return jnp.logical_or(step == 0, jnp.logical_and(odd, step < blocks - 1))

    def turn_at(step):
        return jnp.where(for_partner(step), lax.div(step + 1, 2), lax.div(jnp.maximum(step - 1, 0), 2))

    def block_at(step):
        side = jnp.where(for_partner(step), 1 - col, col)
        return 2 * level_at(turn_at(step)) + side

    barrier = pltpu.get_barrier_semaphore()
    for index in (left, right):
        pl.semaphore_signal(barrier, inc=1, device_id=peer("chan", index), device_id_type=MESH)
    greeted = 2
    if scatter:
        partner = me + 1 - 2 * col
        pl.semaphore_signal(barrier, inc=1, device_id=peer("obs", partner), device_id_type=MESH)
        for turn in range(pairs - 1):
            index = 2 * level_at(turn) + col
            pl.semaphore_signal(barrier, inc=1, device_id=peer("obs", index), device_id_type=MESH)
        greeted += pairs

    base = pl.multiple_of(chan * own, own)
    smalls = [
        pltpu.make_async_copy(pred, pred_in, small_sem.at[0]),
        pltpu.make_async_copy(counts, counts_in, small_sem.at[1]),
        pltpu.make_async_copy(inv, inv_in, small_sem.at[2]),
        pltpu.make_async_copy(
            ids.at[:, pl.ds(base, own)], ids_in.at[:, pl.ds(LANES, own)], small_sem.at[3]
        ),
    ]
    before = pltpu.make_async_copy(
        ids.at[:, pl.ds(pl.multiple_of(jnp.maximum(base - LANES, 0), LANES), LANES)],
        ids_in.at[:, pl.ds(0, LANES)],
        small_sem.at[4],
    )
    after = pltpu.make_async_copy(
        ids.at[:, pl.ds(pl.multiple_of(jnp.minimum(base + own, own * n_chan - LANES), LANES), LANES)],
        ids_in.at[:, pl.ds(LANES + own, LANES)],
        small_sem.at[5],
    )
    for copy in smalls:
        copy.start()
    before.start()
    after.start()

    origin = block_at(0) + blocks - jnp.where(stride == 1, 1, blocks - 1)
    hop = jnp.where(stride == 1, 1, blocks - 1)

    def load(place):
        chunk = lax.rem(origin + hop * place, blocks)
        start = pl.multiple_of(chunk * width, width)
        return pltpu.make_async_copy(
            dep.at[pl.ds(start, width), :],
            window.at[pl.ds(start + HALO, width), :],
            load_sem.at[place],
        )

    def start_load(place, carry):
        load(place).start()
        return carry

    lax.fori_loop(0, blocks, start_load, 0)

    smalls[0].wait()
    smalls[1].wait()
    values = pred_in[...].astype(jnp.float32)
    wide[upper + preds :, :] = jnp.zeros((LANES - upper - preds, obs_dev), jnp.float32)
    first_row = 0
    for first in range(preds):
        count = preds - first
        wide[first_row : first_row + count, :] = values[first:, :] * values[first : first + 1, :]
        first_row += count
    wide[upper : upper + preds, :] = values
    lane = lax.broadcasted_iota(jnp.int32, (slots, LANES), 1)

    def turn_line(line, carry):
        at = pl.ds(pl.multiple_of(line * slots, slots), slots)
        slot = lax.broadcasted_iota(jnp.int32, (LANES, slots), 1)
        live = jnp.where(slot < counts_in[line], wide[:, at], 0.0)
        turned = live.T
        per = OBS_CHUNK // slots
        spot_q = pl.multiple_of(lax.div(line, per) * 2 * OBS_CHUNK + lax.rem(line, per) * slots, slots)
        table[pl.ds(spot_q, slots), :] = jnp.where(lane < upper, turned, 0.0).astype(jnp.bfloat16)
        table[pl.ds(spot_q + OBS_CHUNK, slots), :] = jnp.where(lane >= upper, turned, 0.0).astype(
            jnp.bfloat16
        )
        return carry

    lax.fori_loop(0, lines, turn_line, 0, unroll=4)

    pl.semaphore_wait(barrier, greeted)
    to_left = pltpu.make_async_remote_copy(
        src_ref=dep.at[pl.ds(0, HALO), :],
        dst_ref=window.at[pl.ds(own + HALO, HALO), :],
        send_sem=halo_send.at[0],
        recv_sem=halo_recv.at[0],
        device_id=peer("chan", left),
        device_id_type=MESH,
    )
    to_right = pltpu.make_async_remote_copy(
        src_ref=dep.at[pl.ds(own - HALO, HALO), :],
        dst_ref=window.at[pl.ds(0, HALO), :],
        send_sem=halo_send.at[1],
        recv_sem=halo_recv.at[1],
        device_id=peer("chan", right),
        device_id_type=MESH,
    )
    to_left.start()
    to_right.start()

    smalls[2].wait()
    smalls[3].wait()
    before.wait()
    after.wait()

    @pl.when(chan == 0)
    def _():
        ids_in[:, 0:LANES] = jnp.full((1, LANES), -1, jnp.int32)

    @pl.when(chan == n_chan - 1)
    def _():
        ids_in[:, LANES + own :] = jnp.full((1, LANES), -1, jnp.int32)

    flip[...] = jnp.zeros_like(flip)

    def build(block):
        for part in range(tiles):
            first = pl.multiple_of(block * width + part * TILE, TILE)
            near = ids_in[:, pl.ds(first, 3 * TILE)].astype(jnp.float32)
            flip[part, 0:offsets, :] = inv_in[:, pl.ds(first, TILE)].astype(jnp.float32)
            flip[part, 64:65, :] = near[:, TILE : 2 * TILE]
            turned = flip[part].T
            own_id = turned[:, 64:65]
            place = lax.broadcasted_iota(jnp.int32, turned.shape, 1)
            turned = jnp.where(place < offsets, turned, 0.0)
            skewed = pltpu.roll(
                jnp.concatenate([turned, jnp.zeros_like(turned)], axis=1),
                HALO - half,
                1,
                stride=1,
                stride_axis=0,
            )
            same = near[:, TILE - HALO : 3 * TILE - HALO] == own_id
            bands[part * TILE : (part + 1) * TILE, :] = jnp.where(same, skewed, 0.0).astype(
                jnp.bfloat16
            )

    def send_x(turn):
        return pltpu.make_async_remote_copy(
            src_ref=stage.at[turn],
            dst_ref=landed_x.at[turn],
            send_sem=x_send.at[turn],
            recv_sem=x_recv.at[turn],
            device_id=peer("obs", partner),
            device_id_type=MESH,
        )

    def send_z(turn):
        return pltpu.make_async_remote_copy(
            src_ref=stage.at[pairs + turn],
            dst_ref=landed_z.at[lev],
            send_sem=z_send.at[turn],
            recv_sem=z_recv.at[lev],
            device_id=peer("obs", 2 * level_at(turn) + col),
            device_id_type=MESH,
        )

    def from_z(turn):
        sender = level_at(turn)
        return pltpu.make_async_remote_copy(
            src_ref=stage.at[pairs],
            dst_ref=landed_z.at[sender],
            send_sem=z_send.at[0],
            recv_sem=z_recv.at[sender],
            device_id=peer("obs", 2 * sender + col),
            device_id_type=MESH,
        )

    for place in range(3):
        load(place).wait()
    build(block_at(0))

    def one_block(step, carry):
        block = block_at(step)

        @pl.when(step == 1)
        def _():
            for place in range(3, 5):
                load(place).wait()

        @pl.when(step == 2)
        def _():
            for place in range(5, blocks):
                load(place).wait()

        @pl.when(block == blocks - 1)
        def _():
            to_left.wait_recv()

        @pl.when(block == 0)
        def _():
            to_right.wait_recv()

        start = pl.multiple_of(block * width, width)
        extent = TILE + 2 * HALO
        sums = jnp.zeros((width, LANES), jnp.float32)
        matrices = [bands[part * TILE : (part + 1) * TILE, 0:extent] for part in range(tiles)]
        for at in range(0, obs_dev, OBS_CHUNK):
            parts = []
            for part in range(tiles):
                first = pl.multiple_of(start + part * TILE, TILE)
                weighted = jnp.dot(
                    matrices[part],
                    window[pl.ds(first, extent), at : at + OBS_CHUNK],
                    preferred_element_type=jnp.float32,
                )
                ratio = huber_edge / jnp.maximum(jnp.abs(weighted), huber_edge)
                qc_weight = ratio.astype(jnp.bfloat16)
                scaled = jnp.clip(weighted, -huber_edge, huber_edge).astype(jnp.bfloat16)
                parts.append(jnp.concatenate([qc_weight, scaled], axis=1))
            sums += jnp.dot(
                jnp.concatenate(parts, axis=0),
                table[2 * at : 2 * (at + OBS_CHUNK), :],
                preferred_element_type=jnp.float32,
            )
        build(block_at(jnp.minimum(step + 1, blocks - 1)))
        result = sums.T[:rows, :]
        if not scatter:
            part_out[:, pl.ds(start, width)] = result
            return carry
        turn = turn_at(step)

        @pl.when(for_partner(step))
        def _():
            stage[turn] = result
            send_x(turn).start()

        @pl.when(jnp.logical_not(for_partner(step)))
        def _():
            send_x(turn).wait_recv()
            stage[pairs + turn] = result + landed_x[turn]

            @pl.when(step < blocks - 1)
            def _():
                send_z(turn).start()

        return carry

    lax.fori_loop(0, blocks, one_block, 0)
    to_left.wait_send()
    to_right.wait_send()

    if scatter:
        sums = stage[blocks - 1]
        for turn in range(pairs - 2, -1, -1):
            from_z(turn).wait_recv()
            sums = sums + landed_z[level_at(turn)]
        total[...] = sums * (1.0 / float(obs_dev * n_obs))
        for row, source in enumerate(mirror_rows(preds)):
            gram_out[row : row + 1, :] = total[source : source + 1, :]
        rhs_out[...] = total[upper : upper + preds, :]
        for turn in range(pairs):
            send_x(turn).wait_send()
        for turn in range(pairs - 1):
            send_z(turn).wait_send()


def on_device(departures, predictors, inv_band, band_id, line_counts):
    own, obs_dev = departures.shape
    preds = predictors.shape[0]
    upper = preds * (preds + 1) // 2
    n_obs = lax.axis_size("obs")
    n_chan = lax.axis_size("chan")
    share = own // n_obs
    scatter = share % TILE == 0 and n_obs % 2 == 0
    blocks = n_obs if scatter else own // (2 * TILE)
    width = own // blocks
    rows = -(-(upper + preds) // 8) * 8
    if scatter:
        out_shape = (
            pltpu.VMEM((preds * preds, share), jnp.float32),
            pltpu.VMEM((preds, share), jnp.float32),
        )
    else:
        out_shape = (jax.ShapeDtypeStruct((rows, own), jnp.float32),)
    vmem = pl.BlockSpec(memory_space=pltpu.VMEM)
    hbm = pl.BlockSpec(memory_space=pltpu.HBM)
    pairs = blocks // 2
    landing = (pairs, rows, width) if scatter else (1, 8, LANES)
    dma = pltpu.SemaphoreType.DMA
    outs = pl.pallas_call(
        functools.partial(kernel, n_obs, n_chan, scatter),
        out_shape=out_shape,
        in_specs=[hbm] * 5,
        out_specs=tuple(vmem for _ in out_shape),
        scratch_shapes=[
            pltpu.VMEM((own + 2 * HALO, obs_dev), jnp.bfloat16),
            pltpu.VMEM(predictors.shape, jnp.bfloat16),
            pltpu.VMEM(inv_band.shape, jnp.bfloat16),
            pltpu.VMEM((1, own + 2 * LANES), jnp.int32),
            pltpu.SMEM(line_counts.shape, jnp.int32),
            pltpu.VMEM((LANES, obs_dev), jnp.float32),
            pltpu.VMEM((2 * obs_dev, LANES), jnp.bfloat16),
            pltpu.VMEM((width // TILE, LANES, TILE), jnp.float32),
            pltpu.VMEM((width, 2 * TILE), jnp.bfloat16),
            pltpu.VMEM((blocks, rows, width), jnp.float32),
            pltpu.VMEM(landing, jnp.float32),
            pltpu.VMEM(landing, jnp.float32),
            pltpu.VMEM((rows, width), jnp.float32),
            dma((6,)),
            dma((blocks,)),
            dma((2,)),
            dma((2,)),
            dma((pairs,)),
            dma((pairs,)),
            dma((pairs,)),
            dma((pairs,)),
        ],
        compiler_params=pltpu.CompilerParams(
            collective_id=0,
            has_side_effects=True,
            vmem_limit_bytes=67043328 - 120 * 1024,
        ),
        name="normal_equations",
    )(departures, predictors, inv_band, band_id[None, :], line_counts)
    if scatter:
        return outs[0], outs[1]
    factor = 1.0 / float(obs_dev * n_obs)
    part = lax.psum_scatter(outs[0], "obs", scatter_dimension=1, tiled=True) * factor
    mirror = np.array(mirror_rows(preds))
    return part[mirror], part[upper : upper + preds]


def solution(mesh):
    in_specs = (P("chan", "obs"), P(None, "obs"), P(None, "chan"), P(), P("obs"))
    out_specs = (P(None, ("chan", "obs")), P(None, ("chan", "obs")))
    return jax.shard_map(
        on_device, mesh=mesh, in_specs=in_specs, out_specs=out_specs, check_vma=False
    )
```
